32 devices in a mesh: ens: 2 (over y), gx: 16 (over z, x, core).
Axes of the slice: x: 2, y: 2, z: 4, core: 2. Of those that a mesh axis runs over, the one named last changes fastest.
Arguments:
- model_state: float32 [8, 4, 320, 2560], P('ens', None, 'gx'), parts along dimension 0, may hold values from -6 to 6
- driving: float32 [8, 4, 320, 2560], P('ens', None, 'gx'), parts along dimension 0, may hold values from -12 to 12
- mode_east: int32 [30], replicated, may hold values from 1 to 60, as said below
- mode_north: int32 [30], replicated, may hold values from 1 to 60, as said below
- level_class: int32 [4], replicated, may hold values from 0 to 7
- nudge_table: float32 [8, 4], replicated, may hold values from 0.05 to 0.5
Outputs:
- nudged: float32 [8, 4, 320, 2560], P('ens', None, 'gx'), parts along dimension 0
- residual_log: float32 [8, 4], P('ens'), parts along dimension 0
The draws below stay inside these ranges and needn't reach their ends.
There are 2 independent parts, one for each index of `ens`. The reference program is written for one: setup_inputs(seed, part) draws one part's arguments, and reference() takes and returns one part's arrays. A program takes and returns all parts, laid end to end along the dimension named above; an argument that names none is the same for every part. Nothing has to cross between parts.
Inputs may be any that keep to these rules, and one draw needn't show every extreme that they name: `mode_east`: 30 distinct wavenumbers in increasing order, the first 1 and the last 60. `mode_north`: 30 distinct wavenumbers in increasing order, the first 1 and the last 60.
All inputs are finite; a program needn't handle non-finite values.
Results may differ from the reference program's by a relative error of at most 0.0001.
Values sent between devices are 32-bit elements; how exact they have to be, the bound alone decides.
A program may use at most 128 MiB of HBM per device.

```python
import math
import jax
import jax.numpy as jnp
from jax import lax

F = 4
KX = 30
KY = 30
ITERS = 4
NTAB = 8
LEV = 4
NY = 2560
NX = 320


def pick_modes(key, offset_salt, mode_count):
    chosen = jax.random.permutation(jax.random.fold_in(key, offset_salt), 2 * mode_count - 2)[:mode_count - 2] + 2
    first_one = jnp.array([1], jnp.int32)
    last_one = jnp.array([2 * mode_count], jnp.int32)
    return jnp.sort(jnp.concatenate([first_one, chosen.astype(jnp.int32), last_one]))


def draw_mode_east(key, part):
    return pick_modes(key, 11, KX)


def draw_mode_north(key, part):
    return pick_modes(key, 23, KY)


def draw_driving(key, part):
    rough_key, amp_key = jax.random.split(jax.random.fold_in(key, 37), 2)
    full_shape = (F, LEV, NX, NY)
    east_pos = jnp.arange(NX, dtype=jnp.float32)
    north_pos = jnp.arange(NY, dtype=jnp.float32)
    rising = jnp.sqrt(1.0 + 2.0 * east_pos / max(NX - 1, 1))[None, None, :, None]
    wave_nums = jnp.arange(1, 17, dtype=jnp.float32)
    east_table = jnp.sin(jnp.pi * wave_nums[:, None] * (east_pos[None, :] + 1.0) / (NX + 1))
    north_table = jnp.sin(jnp.pi * wave_nums[:, None] * (north_pos[None, :] + 1.0) / (NY + 1))
    amplitudes = jax.random.uniform(amp_key, (F, LEV, 16, 16), jnp.float32, -0.25, 0.25)
    smooth = jnp.einsum('flab,ax,by->flxy', amplitudes, east_table, north_table)
    rough = jnp.clip(jax.random.normal(rough_key, full_shape, jnp.float32), -5.0, 5.0)
    result = rough * rising + smooth
    return jnp.clip(result, -12.0, 12.0)


def with_ends(entries, stream_key, low, top_value):
    longest = entries.shape.index(max(entries.shape))
    spots = []
    for shift in (0, 1):
        where = [jax.random.randint(jax.random.fold_in(stream_key, axis), (), 0, length) for axis, length in enumerate(entries.shape)]
        where[longest] = (where[longest] + shift) % entries.shape[longest]
        spots.append(tuple(where))
    return entries.at[spots[0]].set(low).at[spots[1]].set(top_value)


def steps_of(key, extent, pieces, least, top_value):
    def one(dim, parts):
        draws = jax.random.uniform(jax.random.fold_in(jax.random.fold_in(key, 6), dim), (parts,), jnp.float32, least / len(pieces), top_value / len(pieces))
        return jnp.repeat(jnp.exp(draws), extent[dim] // parts).reshape((-1,) + (1,) * (len(extent) - dim - 1))

    level = one(*pieces[0])
    for cut in pieces[1:]:
        level = level * one(*cut)
    return level


def centred(rng, dims, scale, most, shards=(), kind=jnp.bfloat16):
    drawn = jax.random.normal(rng, dims, jnp.float32) * scale
    if len(shards) > 0:
        drawn = steps_of(rng, dims, shards, -0.22, 0.18) * drawn
    return jnp.clip(drawn, min=-most, max=most).astype(kind)


def setup_inputs(seed: int = 0, part: int = 0) -> dict:
    seeds = jax.random.split(jax.random.key(seed), 7)
    part_keys = jax.random.split(jax.random.fold_in(seeds[6], part), 7)
    return {
        "model_state": centred(part_keys[0], (F, LEV, NX, NY), 1.0, 6.0, ((2, 16),), jnp.float32),
        "driving": draw_driving(jax.random.fold_in(jax.random.fold_in(seeds[6], part), 71), part),
        "mode_east": draw_mode_east(jax.random.fold_in(seeds[6], 71), part),
        "mode_north": draw_mode_north(jax.random.fold_in(seeds[6], 71), part),
        "level_class": with_ends(jax.random.randint(seeds[4], (LEV,), 0, NTAB), jax.random.fold_in(seeds[4], 1), 0, NTAB - 1).astype(jnp.int32),
        "nudge_table": jnp.clip(jnp.exp(jax.random.uniform(seeds[5], (NTAB, F), jnp.float32, math.log(0.05), math.log(0.5))), 0.05, 0.5),
    }


DIFFUSION = 0.24

def sine_table(wavenums, grid_cells):
    places = jnp.arange(1, grid_cells + 1, dtype=jnp.int32)
    phases = wavenums.astype(jnp.int32)[:, None] * places[None, :] % (2 * (grid_cells + 1))
    return jnp.sin(phases.astype(jnp.float32) * (jnp.pi / (grid_cells + 1)))

def reference(model_state, driving, mode_east, mode_north, level_class, nudge_table):
    fields, levels, total_east, north_cells = model_state.shape
    table_east = sine_table(mode_east, total_east)
    table_north = sine_table(mode_north, north_cells)
    weights = nudge_table[level_class].T
    scale_norm = 4.0 / ((total_east + 1) * (north_cells + 1))
    cell_count = float(levels * total_east * north_cells)
    current = model_state
    records = []
    for substep in range(ITERS):
        deviation = driving - current
        along_north = jnp.einsum('flxy,by->flxb', deviation, table_north, precision=lax.Precision.HIGHEST)
        coeffs = jnp.einsum('flxb,ax->flab', along_north, table_east, precision=lax.Precision.HIGHEST) * scale_norm
        partial_value = jnp.einsum('flab,ax->flxb', coeffs, table_east, precision=lax.Precision.HIGHEST)
        tendency = jnp.einsum('flxb,by->flxy', partial_value, table_north, precision=lax.Precision.HIGHEST)
        tendency = tendency * weights[:, :, None, None]
        padded = jnp.pad(current, ((0, 0), (0, 0), (1, 1), (1, 1)))
        stencil = padded[:, :, 2:, 1:-1] + padded[:, :, :-2, 1:-1] + padded[:, :, 1:-1, 2:] + padded[:, :, 1:-1, :-2] - 4.0 * current
        current = current + tendency + DIFFUSION * stencil
        remain = driving - current
        records.append(jnp.sqrt(lax.optimization_barrier(jnp.sum(remain * remain, axis=(1, 2, 3))) / cell_count))
    return (current, jnp.stack(records))
```

```python
import functools
import math

import jax
import jax.numpy as jnp
from jax import lax
from jax.experimental import pallas as pl
from jax.experimental.pallas import tpu as pltpu
from jax.sharding import PartitionSpec as P

ITERS = 4
DIFFUSION = 0.24
LANES = 128
MESH = pl.DeviceIdType.MESH
F32 = jnp.float32
BF16 = jnp.bfloat16


def split2(value):
    high = value.astype(BF16)
    return high, (value - high.astype(F32)).astype(BF16)


def sine_of(product, half_period):
    turns = jnp.floor(product * (0.5 / half_period))
    rest = product - turns * (2.0 * half_period) - half_period
    size = jnp.abs(rest)
    fold = jnp.minimum(size, half_period - size) * (math.pi / half_period)
    x = jnp.where(rest > 0, -fold, fold)
    y = x * x
    tail = -1.0 / 6 + y * (1.0 / 120 + y * (-1.0 / 5040 + y * (1.0 / 362880 - y / 39916800)))
    return x + x * (y * tail)


def kernel(
    n, norm, state, drive, modes_e, modes_n, classes, table, out, stat,
    buf_a, buf_b, drv, nproj, csend, crecv, qbuf, sacc, sbuf, tab, east,
    load_sem, out_sem, halo_send, halo_recv, ex_send, ex_recv,
):
    fields, cols, levels, ny = state.shape
    nf = fields * levels
    kx, ky = modes_e.shape[0], modes_n.shape[0]
    nx = cols * n
    pairs = east.shape[0]
    rows_each = csend.shape[1]
    per = nf // rows_each
    h = ITERS
    ext = cols + 2 * h
    me = lax.axis_index("gx")
    has_left, has_right = me > 0, me < n - 1
    inner = pl.ds(LANES, ny)

    barrier = pltpu.get_barrier_semaphore()

    def greet(d, carry):
        pl.semaphore_signal(
            barrier, inc=1, device_id={"gx": lax.rem(me + d, n)}, device_id_type=MESH
        )
        return carry

    lax.fori_loop(1, n, greet, 0)

    for f in range(fields):
        of_f = pl.ds(f * levels, levels)
        pltpu.make_async_copy(
            state.at[f], buf_a.at[pl.ds(h, cols), of_f, inner], load_sem.at[0]
        ).start()
    for f in range(fields):
        of_f = pl.ds(f * levels, levels)
        pltpu.make_async_copy(drive.at[f], drv.at[:, of_f], load_sem.at[1]).start()

    guard = jnp.zeros((ext, nf, LANES), F32)
    for buf in (buf_a, buf_b):
        buf[:, :, 0:LANES] = guard
        buf[:, :, ny + LANES : ny + 2 * LANES] = guard

    line = lax.broadcasted_iota(jnp.int32, (32, LANES), 0)
    wave = jnp.zeros((32, LANES), F32)
    for b in range(ky):
        wave = jnp.where(line == b, modes_n[b].astype(F32), wave)
    place = lax.broadcasted_iota(jnp.int32, (32, LANES), 1).astype(F32) + 1.0

    def north_block(k, carry):
        at = pl.ds(pl.multiple_of(k * LANES, LANES), LANES)
        first = (k * LANES).astype(F32)
        high, low = split2(sine_of(wave * (place + first), ny + 1))
        tab[:, at] = jnp.concatenate([high, high, low, low], axis=0)
        return carry

    lax.fori_loop(0, ny // LANES, north_block, 0)

    spot = (lax.broadcasted_iota(jnp.int32, (cols, LANES), 0) + (me * cols + 1)).astype(F32)
    half = lax.broadcasted_iota(jnp.int32, (cols, LANES), 1) // 64
    for p in range(pairs):
        waves = [modes_e[a].astype(F32) if a < kx else 0.0 for a in (2 * p, 2 * p + 1)]
        east[p] = sine_of(jnp.where(half == 0, waves[0], waves[1]) * spot, nx + 1)

    own = buf_a.at[pl.ds(h, cols), :, inner]
    pltpu.make_async_copy(own, own, load_sem.at[0]).wait()
    pl.semaphore_wait(barrier, n - 1)

    def halo(src_row, dst_row, target, side):
        return pltpu.make_async_remote_copy(
            src_ref=buf_a.at[pl.ds(src_row, h), :, inner],
            dst_ref=buf_a.at[pl.ds(dst_row, h), :, inner],
            send_sem=halo_send.at[side],
            recv_sem=halo_recv.at[side],
            device_id={"gx": target},
            device_id_type=MESH,
        )

    to_right = halo(cols, 0, lax.rem(me + 1, n), 0)
    to_left = halo(h, h + cols, lax.rem(me + n - 1, n), 1)

    @pl.when(has_right)
    def _():
        to_right.start()

    @pl.when(has_left)
    def _():
        to_left.start()

    @pl.when(jnp.logical_not(has_left))
    def _():
        buf_a[h - 1, :, inner] = jnp.zeros((nf, ny), F32)
        for k in range(1, h):
            buf_a[h - 1 - k, :, inner] = -buf_a[h - 1 + k, :, inner]

    @pl.when(jnp.logical_not(has_right))
    def _():
        edge = h + cols
        buf_a[edge, :, inner] = jnp.zeros((nf, ny), F32)
        for k in range(1, h):
            buf_a[edge + k, :, inner] = -buf_a[edge - k, :, inner]

    kc = 512 if ny % 512 == 0 else LANES

    def project(load):
        total = jnp.zeros((2 * cols * nf, LANES), F32)
        for c in range(ny // kc):
            high, low = split2(load(c * kc).reshape(cols * nf, kc))
            total += lax.dot_general(
                jnp.concatenate([high, low], axis=0),
                tab[:, c * kc : (c + 1) * kc],
                (((1,), (1,)), ((), ())),
                preferred_element_type=F32,
            )
        both = total[: cols * nf] + total[cols * nf :]
        return both + pltpu.roll(both, 64, 1)

    proj_u = project(lambda k: buf_a[h : h + cols, :, LANES + k : LANES + k + kc])
    pltpu.make_async_copy(drv, drv, load_sem.at[1]).wait()
    proj_d = project(lambda k: drv[:, :, k : k + kc])
    group = lax.broadcasted_iota(jnp.int32, (cols * nf, LANES), 1) // 32 % 2
    nproj[...] = jnp.where(group == 0, proj_d, proj_u).reshape(cols, nf, LANES)

    def east_project(p, carry):
        acc = jnp.zeros((nf, LANES), F32)
        for x in range(cols):
            acc += east[p, x : x + 1, :] * nproj[x]
        for k in range(per):
            csend[p * per + k] = acc[k * rows_each : (k + 1) * rows_each]
        return carry

    lax.fori_loop(0, pairs, east_project, 0)

    def exchange(source, target_slot, idx):
        def one(d, carry):
            t = lax.rem(me + d, n)
            pltpu.make_async_remote_copy(
                src_ref=source(t),
                dst_ref=target_slot(d),
                send_sem=ex_send.at[idx],
                recv_sem=ex_recv.at[idx],
                device_id={"gx": t},
                device_id_type=MESH,
            ).start()
            return carry

        lax.fori_loop(1, n, one, 0)

    def all_of(buf, sem):
        part = buf.at[pl.ds(0, n - 1)]
        pltpu.make_async_copy(part, part, sem).wait()

    exchange(lambda t: csend.at[t], lambda d: crecv.at[d - 1], 0)

    width = ny // 2 if ny % 256 == 0 else ny

    def diffuse(src, dst, reach, index):
        def row(x, acc, counted):
            for c in range(ny // width):
                lo = c * width
                window = src[x, :, lo : lo + width + 2 * LANES]
                left = pltpu.roll(window, 1, 1)[:, LANES:-LANES]
                right = pltpu.roll(window, width + 2 * LANES - 1, 1)[:, LANES:-LANES]
                mid = slice(lo + LANES, lo + LANES + width)
                sides = (left + right) + (src[x - 1, :, mid] + src[x + 1, :, mid])
                new = (1.0 - 4.0 * DIFFUSION) * window[:, LANES:-LANES] + DIFFUSION * sides
                dst[x, :, mid] = new
                if counted:
                    gap = drv[x - h, :, lo : lo + width] - new
                    gap = gap * gap
                    for t in range(width // LANES):
                        acc += gap[:, t * LANES : (t + 1) * LANES]
            return acc

        zero = jnp.zeros((nf, LANES), F32)
        if reach > 0:
            lax.fori_loop(h - reach, h, lambda x, a: row(x, a, False), zero)
            lax.fori_loop(h + cols, h + cols + reach, lambda x, a: row(x, a, False), zero)
        sacc[index] = lax.fori_loop(h, h + cols, lambda x, a: row(x, a, True), zero)

    @pl.when(has_left)
    def _():
        to_right.wait_recv()

    @pl.when(has_right)
    def _():
        to_left.wait_recv()

    diffuse(buf_a, buf_b, 3, 0)

    @pl.when(has_right)
    def _():
        to_right.wait_send()

    @pl.when(has_left)
    def _():
        to_left.wait_send()

    diffuse(buf_b, buf_a, 2, 1)

    all_of(crecv, ex_recv.at[0])
    mine = lax.fori_loop(0, n - 1, lambda k, a: a + crecv[k], csend[me]) * norm
    lane = lax.broadcasted_iota(jnp.int32, (rows_each, LANES), 1)
    target = jnp.where(lane // 32 % 2 == 0, mine, 0.0)
    start = jnp.where(lane // 32 % 2 == 0, pltpu.roll(mine, LANES - 32, 1), 0.0)
    pair = me // per
    entry = lax.broadcasted_iota(jnp.int32, (rows_each, LANES), 0) + me % per * rows_each
    first, second = (modes_e[jnp.minimum(2 * pair + k, kx - 1)].astype(F32) for k in (0, 1))
    wave_e = jnp.where(lane < 64, first, second)
    wave_n = jnp.zeros((rows_each, LANES), F32)
    for b in range(ky):
        wave_n = jnp.where(lane % 32 == b, modes_n[b].astype(F32), wave_n)
    damp = sine_of(wave_e, 2 * (nx + 1)) ** 2 + sine_of(wave_n, 2 * (ny + 1)) ** 2
    mu = 1.0 - 4.0 * DIFFUSION * damp
    w = jnp.zeros((rows_each, LANES), F32)
    for f in range(fields):
        for l in range(levels):
            w = jnp.where(entry == f * levels + l, table[f, classes[l]], w)
    valid = (2 * pair + lane // 64 < kx) & (lane % 64 < ky)
    w = jnp.where(valid, w, 0.0)
    q = jnp.zeros_like(target)
    free = start
    fixes = []
    for s in range(ITERS):
        q = mu * q + w * (target - (free + q))
        free = mu * free
        fixes.append(q * (q - 2.0 * (target - free)) * (1.0 / norm))
    qbuf[me] = q
    exchange(lambda t: qbuf.at[me], lambda d: qbuf.at[me], 1)

    diffuse(buf_a, buf_b, 1, 2)
    diffuse(buf_b, buf_a, 0, 3)

    lane = lax.broadcasted_iota(jnp.int32, (8, LANES), 1)
    line = lax.broadcasted_iota(jnp.int32, (8, LANES), 0)
    owner = lax.broadcasted_iota(jnp.int32, (nf, LANES), 0) // levels
    local = jnp.zeros((8, LANES), F32)
    for s in range(ITERS):
        for f in range(fields):
            both = jnp.sum(jnp.where(owner == f, sacc[s], 0.0), axis=0, keepdims=True)
            both += jnp.sum(
                jnp.where(entry // levels == f, fixes[s], 0.0), axis=0, keepdims=True
            )
            both = jnp.sum(both, axis=1, keepdims=True)
            local = jnp.where((line == s) & (lane == f), both, local)
    sbuf[me] = local
    exchange(lambda t: sbuf.at[me], lambda d: sbuf.at[me], 2)

    all_of(qbuf, ex_recv.at[1])

    def rebuild(x, carry):
        acc = jnp.zeros((nf, LANES), F32)
        for p in range(pairs):
            if per == 1:
                rows = qbuf[p]
            else:
                rows = jnp.concatenate([qbuf[p * per + k] for k in range(per)], axis=0)
            acc += east[p, pl.ds(x, 1), :] * rows
        nproj[x] = acc + pltpu.roll(acc, 64, 1)
        return carry

    lax.fori_loop(0, cols, rebuild, 0)
    step = 4 if cols % 4 == 0 else 1
    lane = lax.broadcasted_iota(jnp.int32, (step * nf, LANES), 1)
    for g in range(cols // step):
        coeff = nproj[g * step : (g + 1) * step].reshape(step * nf, LANES)
        rest = coeff - coeff.astype(BF16).astype(F32)
        lhs = jnp.where(lane // 32 % 2 == 0, coeff, pltpu.roll(rest, 32, 1)).astype(BF16)
        for c in range(ny // kc):
            sl = slice(c * kc, (c + 1) * kc)
            part = jnp.dot(lhs, tab[:, sl], preferred_element_type=F32)
            drv[g * step : (g + 1) * step, :, sl] = (
                part.reshape(step, nf, kc)
                + buf_a[h + g * step : h + (g + 1) * step, :, LANES + c * kc : LANES + (c + 1) * kc]
            )
        some = pl.ds(g * step, step)
        for f in range(fields):
            pltpu.make_async_copy(
                drv.at[some, pl.ds(f * levels, levels)], out.at[f, some], out_sem
            ).start()

    all_of(sbuf, ex_recv.at[2])
    squares = lax.fori_loop(1, n, lambda k, a: a + sbuf[k], sbuf[0])
    cells = float(levels * nx * ny)
    stat[...] = jnp.sqrt(jnp.maximum(squares[:ITERS, :fields], 0.0) / cells)
    all_of(crecv, ex_send.at[0])
    all_of(qbuf, ex_send.at[1])
    all_of(sbuf, ex_send.at[2])
    pltpu.make_async_copy(drv, drv, out_sem).wait()


def local(model_state, driving, mode_east, mode_north, level_class, nudge_table):
    fields, levels, cols, ny = model_state.shape
    nf = fields * levels
    n = lax.axis_size("gx")
    nx = cols * n
    norm = 4.0 / ((nx + 1) * (ny + 1))
    pairs = 16
    rows_each = pairs * nf // n
    ext = cols + 2 * ITERS
    any_space = pl.BlockSpec(memory_space=pl.ANY)
    vmem = pl.BlockSpec(memory_space=pltpu.VMEM)
    smem = pl.BlockSpec(memory_space=pltpu.SMEM)
    out, stat = pl.pallas_call(
        functools.partial(kernel, n, norm),
        out_shape=(
            jax.ShapeDtypeStruct((fields, cols, levels, ny), F32),
            jax.ShapeDtypeStruct((ITERS, fields), F32),
        ),
        in_specs=[any_space, any_space, smem, smem, smem, smem],
        out_specs=(any_space, vmem),
        scratch_shapes=[
            pltpu.VMEM((ext, nf, ny + 2 * LANES), F32),
            pltpu.VMEM((ext, nf, ny + 2 * LANES), F32),
            pltpu.VMEM((cols, nf, ny), F32),
            pltpu.VMEM((cols, nf, LANES), F32),
            pltpu.VMEM((n, rows_each, LANES), F32),
            pltpu.VMEM((n, rows_each, LANES), F32),
            pltpu.VMEM((n, rows_each, LANES), F32),
            pltpu.VMEM((ITERS, nf, LANES), F32),
            pltpu.VMEM((n, 8, LANES), F32),
            pltpu.VMEM((LANES, ny), BF16),
            pltpu.VMEM((pairs, cols, LANES), F32),
            pltpu.SemaphoreType.DMA((2,)),
            pltpu.SemaphoreType.DMA,
            pltpu.SemaphoreType.DMA((2,)),
            pltpu.SemaphoreType.DMA((2,)),
            pltpu.SemaphoreType.DMA((3,)),
            pltpu.SemaphoreType.DMA((3,)),
        ],
        compiler_params=pltpu.CompilerParams(collective_id=0, has_side_effects=True),
    )(
        model_state.transpose(0, 2, 1, 3),
        driving.transpose(0, 2, 1, 3),
        mode_east, mode_north, level_class, nudge_table.T,
    )
    return out.transpose(0, 2, 1, 3), stat


def solution(mesh):
    return jax.shard_map(
        local,
        mesh=mesh,
        in_specs=(P("ens", None, "gx", None), P("ens", None, "gx", None), P(), P(), P(), P()),
        out_specs=(P("ens", None, "gx", None), P("ens", None)),
        check_vma=False,
    )
```

```python
import functools
import math

import jax
import jax.numpy as jnp
from jax import lax
from jax.experimental import pallas as pl
from jax.experimental.pallas import tpu as pltpu
from jax.sharding import PartitionSpec as P

ITERS = 4
DIFFUSION = 0.24
LANES = 128
MESH = pl.DeviceIdType.MESH
F32 = jnp.float32
BF16 = jnp.bfloat16


def split2(value):
    high = value.astype(BF16)
    return high, (value - high.astype(F32)).astype(BF16)


def sine_of(product, half_period):
    turns = jnp.floor(product * (0.5 / half_period))
    rest = product - turns * (2.0 * half_period) - half_period
    size = jnp.abs(rest)
    fold = jnp.minimum(size, half_period - size) * (math.pi / half_period)
    x = jnp.where(rest > 0, -fold, fold)
    y = x * x
    tail = -1.0 / 6 + y * (1.0 / 120 + y * (-1.0 / 5040 + y * (1.0 / 362880 - y / 39916800)))
    return x + x * (y * tail)


def kernel(
    n, norm, state, drive, modes_e, modes_n, classes, table, free_out, nproj, tab, stat,
    buf_a, buf_b, drv, csend, crecv, qbuf, sacc, sbuf, east,
    load_sem, out_sem, halo_send, halo_recv, ex_send, ex_recv,
):
    fields, cols, levels, ny = state.shape
    nf = fields * levels
    kx, ky = modes_e.shape[0], modes_n.shape[0]
    nx = cols * n
    pairs = east.shape[0]
    rows_each = csend.shape[1]
    per = nf // rows_each
    h = ITERS
    ext = cols + 2 * h
    me = lax.axis_index("gx")
    has_left, has_right = me > 0, me < n - 1
    inner = pl.ds(LANES, ny)

    barrier = pltpu.get_barrier_semaphore()

    def greet(d, carry):
        pl.semaphore_signal(
            barrier, inc=1, device_id={"gx": lax.rem(me + d, n)}, device_id_type=MESH
        )
        return carry

    lax.fori_loop(1, n, greet, 0)

    for f in range(fields):
        of_f = pl.ds(f * levels, levels)
        pltpu.make_async_copy(
            state.at[f], buf_a.at[pl.ds(h, cols), of_f, inner], load_sem.at[0]
        ).start()
    for f in range(fields):
        of_f = pl.ds(f * levels, levels)
        pltpu.make_async_copy(drive.at[f], drv.at[:, of_f], load_sem.at[1]).start()

    guard = jnp.zeros((ext, nf, LANES), F32)
    for buf in (buf_a, buf_b):
        buf[:, :, 0:LANES] = guard
        buf[:, :, ny + LANES : ny + 2 * LANES] = guard

    pl.semaphore_wait(barrier, n - 1)

    def halo(src_row, dst_row, target, side):
        for f in range(fields):
            pltpu.make_async_remote_copy(
                src_ref=state.at[f, pl.ds(src_row, h)],
                dst_ref=buf_a.at[pl.ds(dst_row, h), pl.ds(f * levels, levels), inner],
                send_sem=halo_send.at[side],
                recv_sem=halo_recv.at[side],
                device_id={"gx": target},
                device_id_type=MESH,
            ).start()

    @pl.when(has_right)
    def _():
        halo(cols - h, 0, lax.rem(me + 1, n), 0)

    @pl.when(has_left)
    def _():
        halo(0, h + cols, lax.rem(me + n - 1, n), 1)

    def halo_done(row, sem):
        part = buf_a.at[pl.ds(row, h), :, inner]
        pltpu.make_async_copy(part, part, sem).wait()

    line = lax.broadcasted_iota(jnp.int32, (32, LANES), 0)
    wave = jnp.zeros((32, LANES), F32)
    for b in range(ky):
        wave = jnp.where(line == b, modes_n[b].astype(F32), wave)
    place = lax.broadcasted_iota(jnp.int32, (32, LANES), 1).astype(F32) + 1.0

    def north_block(k, carry):
        at = pl.ds(pl.multiple_of(k * LANES, LANES), LANES)
        first = (k * LANES).astype(F32)
        high, low = split2(sine_of(wave * (place + first), ny + 1))
        tab[:, at] = jnp.concatenate([high, high, low, low], axis=0)
        return carry

    lax.fori_loop(0, ny // LANES, north_block, 0)

    spot = (lax.broadcasted_iota(jnp.int32, (cols, LANES), 0) + (me * cols + 1)).astype(F32)
    half = lax.broadcasted_iota(jnp.int32, (cols, LANES), 1) // 64
    for p in range(pairs):
        waves = [modes_e[a].astype(F32) if a < kx else 0.0 for a in (2 * p, 2 * p + 1)]
        east[p] = sine_of(jnp.where(half == 0, waves[0], waves[1]) * spot, nx + 1)

    own = buf_a.at[pl.ds(h, cols), :, inner]
    pltpu.make_async_copy(own, own, load_sem.at[0]).wait()

    @pl.when(jnp.logical_not(has_left))
    def _():
        buf_a[h - 1, :, inner] = jnp.zeros((nf, ny), F32)
        for k in range(1, h):
            buf_a[h - 1 - k, :, inner] = -buf_a[h - 1 + k, :, inner]

    @pl.when(jnp.logical_not(has_right))
    def _():
        edge = h + cols
        buf_a[edge, :, inner] = jnp.zeros((nf, ny), F32)
        for k in range(1, h):
            buf_a[edge + k, :, inner] = -buf_a[edge - k, :, inner]

    kc = 512 if ny % 512 == 0 else LANES

    def project(load):
        total = jnp.zeros((2 * cols * nf, LANES), F32)
        for c in range(ny // kc):
            high, low = split2(load(c * kc).reshape(cols * nf, kc))
            total += lax.dot_general(
                jnp.concatenate([high, low], axis=0),
                tab[:, c * kc : (c + 1) * kc],
                (((1,), (1,)), ((), ())),
                preferred_element_type=F32,
            )
        both = total[: cols * nf] + total[cols * nf :]
        return both + pltpu.roll(both, 64, 1)

    proj_u = project(lambda k: buf_a[h : h + cols, :, LANES + k : LANES + k + kc])
    pltpu.make_async_copy(drv, drv, load_sem.at[1]).wait()
    proj_d = project(lambda k: drv[:, :, k : k + kc])
    group = lax.broadcasted_iota(jnp.int32, (cols * nf, LANES), 1) // 32 % 2
    nproj[...] = jnp.where(group == 0, proj_d, proj_u).reshape(cols, nf, LANES)

    def east_project(p, carry):
        acc = jnp.zeros((nf, LANES), F32)
        for x in range(cols):
            acc += east[p, x : x + 1, :] * nproj[x]
        for k in range(per):
            csend[p * per + k] = acc[k * rows_each : (k + 1) * rows_each]
        return carry

    lax.fori_loop(0, pairs, east_project, 0)

    def exchange(source, target_slot, idx):
        def one(d, carry):
            t = lax.rem(me + d, n)
            pltpu.make_async_remote_copy(
                src_ref=source(t),
                dst_ref=target_slot(d),
                send_sem=ex_send.at[idx],
                recv_sem=ex_recv.at[idx],
                device_id={"gx": t},
                device_id_type=MESH,
            ).start()
            return carry

        lax.fori_loop(1, n, one, 0)

    def all_of(buf, sem):
        part = buf.at[pl.ds(0, n - 1)]
        pltpu.make_async_copy(part, part, sem).wait()

    exchange(lambda t: csend.at[t], lambda d: crecv.at[d - 1], 0)

    width = ny // 2 if ny % 256 == 0 else ny

    def diffuse(src, dst, plain, counted_rows):
        def row(x, acc, counted):
            for c in range(ny // width):
                lo = c * width
                window = src[x, :, lo : lo + width + 2 * LANES]
                left = pltpu.roll(window, 1, 1)[:, LANES:-LANES]
                right = pltpu.roll(window, width + 2 * LANES - 1, 1)[:, LANES:-LANES]
                mid = slice(lo + LANES, lo + LANES + width)
                sides = (left + right) + (src[x - 1, :, mid] + src[x + 1, :, mid])
                new = (1.0 - 4.0 * DIFFUSION) * window[:, LANES:-LANES] + DIFFUSION * sides
                dst[x, :, mid] = new
                if counted:
                    gap = drv[x - h, :, lo : lo + width] - new
                    gap = gap * gap
                    for t in range(width // LANES):
                        acc += gap[:, t * LANES : (t + 1) * LANES]
            return acc

        zero = jnp.zeros((nf, LANES), F32)
        for lo, hi in plain:
            if hi > lo:
                lax.fori_loop(lo, hi, lambda x, a: row(x, a, False), zero)
        total = zero
        for lo, hi in counted_rows:
            total = lax.fori_loop(lo, hi, lambda x, a: row(x, a, True), total)
        return total

    end = h + cols
    for s in range(1, ITERS + 1):
        src, dst = (buf_a, buf_b) if s % 2 else (buf_b, buf_a)
        sacc[s - 1] = diffuse(src, dst, [], [(h + s, end - s)])
    inside = pltpu.make_async_copy(
        buf_a.at[pl.ds(2 * h, cols - 2 * h), :, inner],
        free_out.at[pl.ds(h, cols - 2 * h)],
        out_sem,
    )
    inside.start()

    all_of(crecv, ex_recv.at[0])
    mine = lax.fori_loop(0, n - 1, lambda k, a: a + crecv[k], csend[me]) * norm
    lane = lax.broadcasted_iota(jnp.int32, (rows_each, LANES), 1)
    target = jnp.where(lane // 32 % 2 == 0, mine, 0.0)
    start = jnp.where(lane // 32 % 2 == 0, pltpu.roll(mine, LANES - 32, 1), 0.0)
    pair = me // per
    entry = lax.broadcasted_iota(jnp.int32, (rows_each, LANES), 0) + me % per * rows_each
    first, second = (modes_e[jnp.minimum(2 * pair + k, kx - 1)].astype(F32) for k in (0, 1))
    wave_e = jnp.where(lane < 64, first, second)
    wave_n = jnp.zeros((rows_each, LANES), F32)
    for b in range(ky):
        wave_n = jnp.where(lane % 32 == b, modes_n[b].astype(F32), wave_n)
    damp = sine_of(wave_e, 2 * (nx + 1)) ** 2 + sine_of(wave_n, 2 * (ny + 1)) ** 2
    mu = 1.0 - 4.0 * DIFFUSION * damp
    w = jnp.zeros((rows_each, LANES), F32)
    for f in range(fields):
        for l in range(levels):
            w = jnp.where(entry == f * levels + l, table[f, classes[l]], w)
    valid = (2 * pair + lane // 64 < kx) & (lane % 64 < ky)
    w = jnp.where(valid, w, 0.0)
    q = jnp.zeros_like(target)
    free = start
    fixes = []
    for s in range(ITERS):
        q = mu * q + w * (target - (free + q))
        free = mu * free
        fixes.append(q * (q - 2.0 * (target - free)) * (1.0 / norm))
    qbuf[me] = q
    exchange(lambda t: qbuf.at[me], lambda d: qbuf.at[me], 1)

    @pl.when(has_left)
    def _():
        halo_done(0, halo_recv.at[0])

    @pl.when(has_right)
    def _():
        halo_done(end, halo_recv.at[1])

    for s in range(1, ITERS + 1):
        src, dst = (buf_a, buf_b) if s % 2 else (buf_b, buf_a)
        sacc[s - 1] += diffuse(
            src, dst, [(s, h), (end, end + h - s)], [(h, h + s), (end - s, end)]
        )
    west, east_edge = (
        pltpu.make_async_copy(
            buf_a.at[pl.ds(first, h), :, inner], free_out.at[pl.ds(first - h, h)], out_sem
        )
        for first in (h, end - h)
    )
    west.start()
    east_edge.start()

    lane = lax.broadcasted_iota(jnp.int32, (8, LANES), 1)
    line = lax.broadcasted_iota(jnp.int32, (8, LANES), 0)
    owner = lax.broadcasted_iota(jnp.int32, (nf, LANES), 0) // levels
    local = jnp.zeros((8, LANES), F32)
    for s in range(ITERS):
        for f in range(fields):
            both = jnp.sum(jnp.where(owner == f, sacc[s], 0.0), axis=0, keepdims=True)
            both += jnp.sum(
                jnp.where(entry // levels == f, fixes[s], 0.0), axis=0, keepdims=True
            )
            both = jnp.sum(both, axis=1, keepdims=True)
            local = jnp.where((line == s) & (lane == f), both, local)
    sbuf[me] = local
    exchange(lambda t: sbuf.at[me], lambda d: sbuf.at[me], 2)

    all_of(qbuf, ex_recv.at[1])

    def rebuild(x, carry):
        acc = jnp.zeros((nf, LANES), F32)
        for p in range(pairs):
            if per == 1:
                rows = qbuf[p]
            else:
                rows = jnp.concatenate([qbuf[p * per + k] for k in range(per)], axis=0)
            acc += east[p, pl.ds(x, 1), :] * rows
        nproj[x] = acc + pltpu.roll(acc, 64, 1)
        return carry

    lax.fori_loop(0, cols, rebuild, 0)
    all_of(sbuf, ex_recv.at[2])
    squares = lax.fori_loop(1, n, lambda k, a: a + sbuf[k], sbuf[0])
    stat[...] = squares
    all_of(crecv, ex_send.at[0])
    all_of(qbuf, ex_send.at[1])
    all_of(sbuf, ex_send.at[2])

    @pl.when(has_right)
    def _():
        halo_done(0, halo_send.at[0])

    @pl.when(has_left)
    def _():
        halo_done(end, halo_send.at[1])

    pltpu.make_async_copy(drv, drv, out_sem).wait()


def finish(cells, free, coeffs, tab, squares, out, log, held, load_sem, out_sem):
    fields, cols, levels, ny = out.shape
    nf = fields * levels
    kc = 512 if ny % 512 == 0 else LANES
    step = 4 if cols % 4 == 0 else 1
    groups = cols // step
    loads = [
        pltpu.make_async_copy(
            free.at[pl.ds(g * step, step)], held.at[pl.ds(g * step, step)], load_sem.at[g]
        )
        for g in range(groups)
    ]
    for load in loads:
        load.start()
    log[...] = jnp.sqrt(jnp.maximum(squares[:ITERS, :fields], 0.0) / cells)
    lane = lax.broadcasted_iota(jnp.int32, (step * nf, LANES), 1)
    for g in range(groups):
        coeff = coeffs[g * step : (g + 1) * step].reshape(step * nf, LANES)
        rest = coeff - coeff.astype(BF16).astype(F32)
        lhs = jnp.where(lane // 32 % 2 == 0, coeff, pltpu.roll(rest, 32, 1)).astype(BF16)
        loads[g].wait()
        for c in range(ny // kc):
            sl = slice(c * kc, (c + 1) * kc)
            part = jnp.dot(lhs, tab[:, sl], preferred_element_type=F32)
            held[g * step : (g + 1) * step, :, sl] += part.reshape(step, nf, kc)
        some = pl.ds(g * step, step)
        for f in range(fields):
            pltpu.make_async_copy(
                held.at[some, pl.ds(f * levels, levels)], out.at[f, some], out_sem
            ).start()
    pltpu.make_async_copy(held, held, out_sem).wait()


def local(model_state, driving, mode_east, mode_north, level_class, nudge_table):
    fields, levels, cols, ny = model_state.shape
    nf = fields * levels
    n = lax.axis_size("gx")
    nx = cols * n
    norm = 4.0 / ((nx + 1) * (ny + 1))
    pairs = 16
    rows_each = pairs * nf // n
    ext = cols + 2 * ITERS
    any_space = pl.BlockSpec(memory_space=pl.ANY)
    vmem = pl.BlockSpec(memory_space=pltpu.VMEM)
    smem = pl.BlockSpec(memory_space=pltpu.SMEM)
    free, coeffs, tab, squares = pl.pallas_call(
        functools.partial(kernel, n, norm),
        out_shape=(
            jax.ShapeDtypeStruct((cols, nf, ny), F32),
            jax.ShapeDtypeStruct((cols, nf, LANES), F32),
            jax.ShapeDtypeStruct((LANES, ny), BF16),
            jax.ShapeDtypeStruct((8, LANES), F32),
        ),
        in_specs=[any_space, any_space, smem, smem, smem, smem],
        out_specs=(any_space, vmem, vmem, vmem),
        scratch_shapes=[
            pltpu.VMEM((ext, nf, ny + 2 * LANES), F32),
            pltpu.VMEM((ext, nf, ny + 2 * LANES), F32),
            pltpu.VMEM((cols, nf, ny), F32),
            pltpu.VMEM((n, rows_each, LANES), F32),
            pltpu.VMEM((n, rows_each, LANES), F32),
            pltpu.VMEM((n, rows_each, LANES), F32),
            pltpu.VMEM((ITERS, nf, LANES), F32),
            pltpu.VMEM((n, 8, LANES), F32),
            pltpu.VMEM((pairs, cols, LANES), F32),
            pltpu.SemaphoreType.DMA((2,)),
            pltpu.SemaphoreType.DMA,
            pltpu.SemaphoreType.DMA((2,)),
            pltpu.SemaphoreType.DMA((2,)),
            pltpu.SemaphoreType.DMA((3,)),
            pltpu.SemaphoreType.DMA((3,)),
        ],
        compiler_params=pltpu.CompilerParams(
            collective_id=0, has_side_effects=True, vmem_limit_bytes=60_000_000
        ),
    )(
        model_state.transpose(0, 2, 1, 3),
        driving.transpose(0, 2, 1, 3),
        mode_east, mode_north, level_class, nudge_table.T,
    )
    step = 4 if cols % 4 == 0 else 1
    out, log = pl.pallas_call(
        functools.partial(finish, float(levels * nx * ny)),
        out_shape=(
            jax.ShapeDtypeStruct((fields, cols, levels, ny), F32),
            jax.ShapeDtypeStruct((ITERS, fields), F32),
        ),
        in_specs=[any_space, vmem, vmem, vmem],
        out_specs=(any_space, vmem),
        scratch_shapes=[
            pltpu.VMEM((cols, nf, ny), F32),
            pltpu.SemaphoreType.DMA((cols // step,)),
            pltpu.SemaphoreType.DMA,
        ],
        compiler_params=pltpu.CompilerParams(vmem_limit_bytes=58_000_000),
    )(free, coeffs, tab, squares)
    return out.transpose(0, 2, 1, 3), log


def solution(mesh):
    return jax.shard_map(
        local,
        mesh=mesh,
        in_specs=(P("ens", None, "gx", None), P("ens", None, "gx", None), P(), P(), P(), P()),
        out_specs=(P("ens", None, "gx", None), P("ens", None)),
        check_vma=False,
    )
```

```python
import functools
import math

import jax
import jax.numpy as jnp
from jax import lax
from jax.experimental import pallas as pl
from jax.experimental.pallas import tpu as pltpu
from jax.sharding import PartitionSpec as P

ITERS = 4
DIFFUSION = 0.24
LANES = 128
MESH = pl.DeviceIdType.MESH
F32 = jnp.float32
BF16 = jnp.bfloat16


def split2(value):
    high = value.astype(BF16)
    return high, (value - high.astype(F32)).astype(BF16)


def sine_of(product, half_period):
    turns = jnp.floor(product * (0.5 / half_period))
    rest = product - turns * (2.0 * half_period) - half_period
    size = jnp.abs(rest)
    fold = jnp.minimum(size, half_period - size) * (math.pi / half_period)
    x = jnp.where(rest > 0, -fold, fold)
    y = x * x
    tail = -1.0 / 6 + y * (1.0 / 120 + y * (-1.0 / 5040 + y * (1.0 / 362880 - y / 39916800)))
    return x + x * (y * tail)


def kernel(
    n, norm, state, drive, modes_e, modes_n, classes, table, free_out, nproj, tab, stat,
    buf_a, buf_b, drv, csend, crecv, qbuf, sacc, sbuf, east,
    load_sem, out_sem, halo_send, halo_recv, ex_send, ex_recv,
):
    fields, cols, levels, ny = state.shape
    nf = fields * levels
    kx, ky = modes_e.shape[0], modes_n.shape[0]
    nx = cols * n
    pairs = east.shape[0]
    rows_each = csend.shape[1]
    per = nf // rows_each
    h = ITERS
    ext = cols + 2 * h
    me = lax.axis_index("gx")
    has_left, has_right = me > 0, me < n - 1
    inner = pl.ds(LANES, ny)

    barrier = pltpu.get_barrier_semaphore()

    def greet(d, carry):
        pl.semaphore_signal(
            barrier, inc=1, device_id={"gx": lax.rem(me + d, n)}, device_id_type=MESH
        )
        return carry

    lax.fori_loop(1, n, greet, 0)

    for f in range(fields):
        of_f = pl.ds(f * levels, levels)
        pltpu.make_async_copy(
            state.at[f], buf_a.at[pl.ds(h, cols), of_f, inner], load_sem.at[0]
        ).start()
    for f in range(fields):
        of_f = pl.ds(f * levels, levels)
        pltpu.make_async_copy(drive.at[f], drv.at[:, of_f], load_sem.at[1]).start()

    guard = jnp.zeros((ext, nf, LANES), F32)
    for buf in (buf_a, buf_b):
        buf[:, :, 0:LANES] = guard
        buf[:, :, ny + LANES : ny + 2 * LANES] = guard

    pl.semaphore_wait(barrier, n - 1)

    def halo(src_row, dst_row, target, side, some):
        for f in some:
            pltpu.make_async_remote_copy(
                src_ref=state.at[f, pl.ds(src_row, h)],
                dst_ref=buf_a.at[pl.ds(dst_row, h), pl.ds(f * levels, levels), inner],
                send_sem=halo_send.at[side],
                recv_sem=halo_recv.at[side],
                device_id={"gx": target},
                device_id_type=MESH,
            ).start()

    def halos(some):
        @pl.when(has_right)
        def _():
            halo(cols - h, 0, lax.rem(me + 1, n), 0, some)

        @pl.when(has_left)
        def _():
            halo(0, h + cols, lax.rem(me + n - 1, n), 1, some)

    halos(range(fields // 2))

    def halo_done(row, sem):
        part = buf_a.at[pl.ds(row, h), :, inner]
        pltpu.make_async_copy(part, part, sem).wait()

    line = lax.broadcasted_iota(jnp.int32, (32, LANES), 0)
    wave = jnp.zeros((32, LANES), F32)
    for b in range(ky):
        wave = jnp.where(line == b, modes_n[b].astype(F32), wave)
    place = lax.broadcasted_iota(jnp.int32, (32, LANES), 1).astype(F32) + 1.0

    def north_block(k, carry):
        at = pl.ds(pl.multiple_of(k * LANES, LANES), LANES)
        first = (k * LANES).astype(F32)
        high, low = split2(sine_of(wave * (place + first), ny + 1))
        tab[:, at] = jnp.concatenate([high, high, low, low], axis=0)
        return carry

    lax.fori_loop(0, ny // LANES, north_block, 0)

    spot = (lax.broadcasted_iota(jnp.int32, (cols, LANES), 0) + (me * cols + 1)).astype(F32)
    half = lax.broadcasted_iota(jnp.int32, (cols, LANES), 1) // 64
    for p in range(pairs):
        waves = [modes_e[a].astype(F32) if a < kx else 0.0 for a in (2 * p, 2 * p + 1)]
        east[p] = sine_of(jnp.where(half == 0, waves[0], waves[1]) * spot, nx + 1)

    own = buf_a.at[pl.ds(h, cols), :, inner]
    pltpu.make_async_copy(own, own, load_sem.at[0]).wait()

    @pl.when(jnp.logical_not(has_left))
    def _():
        buf_a[h - 1, :, inner] = jnp.zeros((nf, ny), F32)
        for k in range(1, h):
            buf_a[h - 1 - k, :, inner] = -buf_a[h - 1 + k, :, inner]

    @pl.when(jnp.logical_not(has_right))
    def _():
        edge = h + cols
        buf_a[edge, :, inner] = jnp.zeros((nf, ny), F32)
        for k in range(1, h):
            buf_a[edge + k, :, inner] = -buf_a[edge - k, :, inner]

    kc = 512 if ny % 512 == 0 else LANES

    def project(load):
        total = jnp.zeros((2 * cols * nf, LANES), F32)
        for c in range(ny // kc):
            high, low = split2(load(c * kc).reshape(cols * nf, kc))
            total += lax.dot_general(
                jnp.concatenate([high, low], axis=0),
                tab[:, c * kc : (c + 1) * kc],
                (((1,), (1,)), ((), ())),
                preferred_element_type=F32,
            )
        both = total[: cols * nf] + total[cols * nf :]
        return both + pltpu.roll(both, 64, 1)

    proj_u = project(lambda k: buf_a[h : h + cols, :, LANES + k : LANES + k + kc])
    pltpu.make_async_copy(drv, drv, load_sem.at[1]).wait()
    proj_d = project(lambda k: drv[:, :, k : k + kc])
    group = lax.broadcasted_iota(jnp.int32, (cols * nf, LANES), 1) // 32 % 2
    nproj[...] = jnp.where(group == 0, proj_d, proj_u).reshape(cols, nf, LANES)

    def east_project(p, carry):
        acc = jnp.zeros((nf, LANES), F32)
        for x in range(cols):
            acc += east[p, x : x + 1, :] * nproj[x]
        for k in range(per):
            csend[p * per + k] = acc[k * rows_each : (k + 1) * rows_each]
        return carry

    lax.fori_loop(0, pairs, east_project, 0)

    def exchange(source, target_slot, idx):
        def one(d, carry):
            t = lax.rem(me + d, n)
            pltpu.make_async_remote_copy(
                src_ref=source(t),
                dst_ref=target_slot(d),
                send_sem=ex_send.at[idx],
                recv_sem=ex_recv.at[idx],
                device_id={"gx": t},
                device_id_type=MESH,
            ).start()
            return carry

        lax.fori_loop(1, n, one, 0)

    def all_of(buf, sem):
        part = buf.at[pl.ds(0, n - 1)]
        pltpu.make_async_copy(part, part, sem).wait()

    exchange(lambda t: csend.at[t], lambda d: crecv.at[d - 1], 0)
    halos(range(fields // 2, fields))

    width = ny // 2 if ny % 256 == 0 else ny

    def diffuse(src, dst, plain, counted_rows):
        def row(x, acc, counted):
            for c in range(ny // width):
                lo = c * width
                window = src[x, :, lo : lo + width + 2 * LANES]
                left = pltpu.roll(window, 1, 1)[:, LANES:-LANES]
                right = pltpu.roll(window, width + 2 * LANES - 1, 1)[:, LANES:-LANES]
                mid = slice(lo + LANES, lo + LANES + width)
                sides = (left + right) + (src[x - 1, :, mid] + src[x + 1, :, mid])
                new = (1.0 - 4.0 * DIFFUSION) * window[:, LANES:-LANES] + DIFFUSION * sides
                dst[x, :, mid] = new
                if counted:
                    gap = drv[x - h, :, lo : lo + width] - new
                    gap = gap * gap
                    for t in range(width // LANES):
                        acc += gap[:, t * LANES : (t + 1) * LANES]
            return acc

        zero = jnp.zeros((nf, LANES), F32)
        for lo, hi in plain:
            if hi > lo:
                lax.fori_loop(lo, hi, lambda x, a: row(x, a, False), zero)
        total = zero
        for lo, hi in counted_rows:
            total = lax.fori_loop(lo, hi, lambda x, a: row(x, a, True), total)
        return total

    end = h + cols
    for s in range(1, ITERS + 1):
        src, dst = (buf_a, buf_b) if s % 2 else (buf_b, buf_a)
        sacc[s - 1] = diffuse(src, dst, [], [(h + s, end - s)])
    inside = pltpu.make_async_copy(
        buf_a.at[pl.ds(2 * h, cols - 2 * h), :, inner],
        free_out.at[pl.ds(h, cols - 2 * h)],
        out_sem,
    )
    inside.start()

    all_of(crecv, ex_recv.at[0])
    mine = lax.fori_loop(0, n - 1, lambda k, a: a + crecv[k], csend[me]) * norm
    lane = lax.broadcasted_iota(jnp.int32, (rows_each, LANES), 1)
    target = jnp.where(lane // 32 % 2 == 0, mine, 0.0)
    start = jnp.where(lane // 32 % 2 == 0, pltpu.roll(mine, LANES - 32, 1), 0.0)
    pair = me // per
    entry = lax.broadcasted_iota(jnp.int32, (rows_each, LANES), 0) + me % per * rows_each
    first, second = (modes_e[jnp.minimum(2 * pair + k, kx - 1)].astype(F32) for k in (0, 1))
    wave_e = jnp.where(lane < 64, first, second)
    wave_n = jnp.zeros((rows_each, LANES), F32)
    for b in range(ky):
        wave_n = jnp.where(lane % 32 == b, modes_n[b].astype(F32), wave_n)
    damp = sine_of(wave_e, 2 * (nx + 1)) ** 2 + sine_of(wave_n, 2 * (ny + 1)) ** 2
    mu = 1.0 - 4.0 * DIFFUSION * damp
    w = jnp.zeros((rows_each, LANES), F32)
    for f in range(fields):
        for l in range(levels):
            w = jnp.where(entry == f * levels + l, table[f, classes[l]], w)
    valid = (2 * pair + lane // 64 < kx) & (lane % 64 < ky)
    w = jnp.where(valid, w, 0.0)
    q = jnp.zeros_like(target)
    free = start
    fixes = []
    for s in range(ITERS):
        q = mu * q + w * (target - (free + q))
        free = mu * free
        fixes.append(q * (q - 2.0 * (target - free)) * (1.0 / norm))
    qbuf[me] = q
    exchange(lambda t: qbuf.at[me], lambda d: qbuf.at[me], 1)

    @pl.when(has_left)
    def _():
        halo_done(0, halo_recv.at[0])

    @pl.when(has_right)
    def _():
        halo_done(end, halo_recv.at[1])

    for s in range(1, ITERS + 1):
        src, dst = (buf_a, buf_b) if s % 2 else (buf_b, buf_a)
        sacc[s - 1] += diffuse(
            src, dst, [(s, h), (end, end + h - s)], [(h, h + s), (end - s, end)]
        )
    west, east_edge = (
        pltpu.make_async_copy(
            buf_a.at[pl.ds(first, h), :, inner], free_out.at[pl.ds(first - h, h)], out_sem
        )
        for first in (h, end - h)
    )
    west.start()
    east_edge.start()

    lane = lax.broadcasted_iota(jnp.int32, (8, LANES), 1)
    line = lax.broadcasted_iota(jnp.int32, (8, LANES), 0)
    owner = lax.broadcasted_iota(jnp.int32, (nf, LANES), 0) // levels
    local = jnp.zeros((8, LANES), F32)
    for s in range(ITERS):
        for f in range(fields):
            both = jnp.sum(jnp.where(owner == f, sacc[s], 0.0), axis=0, keepdims=True)
            both += jnp.sum(
                jnp.where(entry // levels == f, fixes[s], 0.0), axis=0, keepdims=True
            )
            both = jnp.sum(both, axis=1, keepdims=True)
            local = jnp.where((line == s) & (lane == f), both, local)
    sbuf[me] = local
    exchange(lambda t: sbuf.at[me], lambda d: sbuf.at[me], 2)

    all_of(qbuf, ex_recv.at[1])

    def rebuild(x, carry):
        acc = jnp.zeros((nf, LANES), F32)
        for p in range(pairs):
            if per == 1:
                rows = qbuf[p]
            else:
                rows = jnp.concatenate([qbuf[p * per + k] for k in range(per)], axis=0)
            acc += east[p, pl.ds(x, 1), :] * rows
        nproj[x] = acc + pltpu.roll(acc, 64, 1)
        return carry

    lax.fori_loop(0, cols, rebuild, 0)
    all_of(sbuf, ex_recv.at[2])
    squares = lax.fori_loop(1, n, lambda k, a: a + sbuf[k], sbuf[0])
    stat[...] = squares
    all_of(crecv, ex_send.at[0])
    all_of(qbuf, ex_send.at[1])
    all_of(sbuf, ex_send.at[2])

    @pl.when(has_right)
    def _():
        halo_done(0, halo_send.at[0])

    @pl.when(has_left)
    def _():
        halo_done(end, halo_send.at[1])

    pltpu.make_async_copy(drv, drv, out_sem).wait()


def finish(cells, free, coeffs, tab, squares, out, log, held, load_sem, out_sem):
    fields, cols, levels, ny = out.shape
    nf = fields * levels
    kc = 512 if ny % 512 == 0 else LANES
    step = 4 if cols % 4 == 0 else 1
    groups = cols // step
    loads = [
        pltpu.make_async_copy(
            free.at[pl.ds(g * step, step)], held.at[pl.ds(g * step, step)], load_sem.at[g]
        )
        for g in range(groups)
    ]
    for load in loads:
        load.start()
    log[...] = jnp.sqrt(jnp.maximum(squares[:ITERS, :fields], 0.0) / cells)
    lane = lax.broadcasted_iota(jnp.int32, (step * nf, LANES), 1)
    for g in range(groups):
        coeff = coeffs[g * step : (g + 1) * step].reshape(step * nf, LANES)
        rest = coeff - coeff.astype(BF16).astype(F32)
        lhs = jnp.where(lane // 32 % 2 == 0, coeff, pltpu.roll(rest, 32, 1)).astype(BF16)
        loads[g].wait()
        for c in range(ny // kc):
            sl = slice(c * kc, (c + 1) * kc)
            part = jnp.dot(lhs, tab[:, sl], preferred_element_type=F32)
            held[g * step : (g + 1) * step, :, sl] += part.reshape(step, nf, kc)
        some = pl.ds(g * step, step)
        for f in range(fields):
            pltpu.make_async_copy(
                held.at[some, pl.ds(f * levels, levels)], out.at[f, some], out_sem
            ).start()
    pltpu.make_async_copy(held, held, out_sem).wait()


def local(model_state, driving, mode_east, mode_north, level_class, nudge_table):
    fields, levels, cols, ny = model_state.shape
    nf = fields * levels
    n = lax.axis_size("gx")
    nx = cols * n
    norm = 4.0 / ((nx + 1) * (ny + 1))
    pairs = 16
    rows_each = pairs * nf // n
    ext = cols + 2 * ITERS
    any_space = pl.BlockSpec(memory_space=pl.ANY)
    vmem = pl.BlockSpec(memory_space=pltpu.VMEM)
    smem = pl.BlockSpec(memory_space=pltpu.SMEM)
    free, coeffs, tab, squares = pl.pallas_call(
        functools.partial(kernel, n, norm),
        out_shape=(
            jax.ShapeDtypeStruct((cols, nf, ny), F32),
            jax.ShapeDtypeStruct((cols, nf, LANES), F32),
            jax.ShapeDtypeStruct((LANES, ny), BF16),
            jax.ShapeDtypeStruct((8, LANES), F32),
        ),
        in_specs=[any_space, any_space, smem, smem, smem, smem],
        out_specs=(any_space, vmem, vmem, vmem),
        scratch_shapes=[
            pltpu.VMEM((ext, nf, ny + 2 * LANES), F32),
            pltpu.VMEM((ext, nf, ny + 2 * LANES), F32),
            pltpu.VMEM((cols, nf, ny), F32),
            pltpu.VMEM((n, rows_each, LANES), F32),
            pltpu.VMEM((n, rows_each, LANES), F32),
            pltpu.VMEM((n, rows_each, LANES), F32),
            pltpu.VMEM((ITERS, nf, LANES), F32),
            pltpu.VMEM((n, 8, LANES), F32),
            pltpu.VMEM((pairs, cols, LANES), F32),
            pltpu.SemaphoreType.DMA((2,)),
            pltpu.SemaphoreType.DMA,
            pltpu.SemaphoreType.DMA((2,)),
            pltpu.SemaphoreType.DMA((2,)),
            pltpu.SemaphoreType.DMA((3,)),
            pltpu.SemaphoreType.DMA((3,)),
        ],
        compiler_params=pltpu.CompilerParams(
            collective_id=0, has_side_effects=True, vmem_limit_bytes=60_000_000
        ),
    )(
        model_state.transpose(0, 2, 1, 3),
        driving.transpose(0, 2, 1, 3),
        mode_east, mode_north, level_class, nudge_table.T,
    )
    step = 4 if cols % 4 == 0 else 1
    out, log = pl.pallas_call(
        functools.partial(finish, float(levels * nx * ny)),
        out_shape=(
            jax.ShapeDtypeStruct((fields, cols, levels, ny), F32),
            jax.ShapeDtypeStruct((ITERS, fields), F32),
        ),
        in_specs=[any_space, vmem, vmem, vmem],
        out_specs=(any_space, vmem),
        scratch_shapes=[
            pltpu.VMEM((cols, nf, ny), F32),
            pltpu.SemaphoreType.DMA((cols // step,)),
            pltpu.SemaphoreType.DMA,
        ],
        compiler_params=pltpu.CompilerParams(vmem_limit_bytes=58_000_000),
    )(free, coeffs, tab, squares)
    return out.transpose(0, 2, 1, 3), log


def solution(mesh):
    return jax.shard_map(
        local,
        mesh=mesh,
        in_specs=(P("ens", None, "gx", None), P("ens", None, "gx", None), P(), P(), P(), P()),
        out_specs=(P("ens", None, "gx", None), P("ens", None)),
        check_vma=False,
    )
```
